32 devices in a mesh: station: 16 (over z, x, core), chan: 2 (over y).
Axes of the slice: x: 2, y: 2, z: 4, core: 2. Of those that a mesh axis runs over, the one named last changes fastest.
Arguments:
- samples: float32 [2, 16, 256, 128, 256], P(None, 'station', 'chan'), may hold values from -6 to 6
- weights: float32 [2, 16, 32, 256, 256], P(None, 'station', None, 'chan'), may hold values from -6 to 6
- antenna_flags: int32 [16, 256], P('station', 'chan'), may hold values from 0 to 1, as said below
- subband_table: int32 [256], replicated, may hold values from 0 to 255, each once
Outputs:
- visibilities: float32 [256, 2, 16, 32, 16], P('chan', None, 'station')
The draws below stay inside these ranges and needn't reach their ends.
Inputs may be any that keep to these rules, and one draw needn't show every extreme that they name: `antenna_flags`: every station has at least 32 antennas with flag 1. `subband_table`: a permutation of 0 to 255.
All inputs are finite; a program needn't handle non-finite values.
Results may differ from the reference program's by a relative error of at most 0.0019.
Values may be sent and summed in bfloat16 or wider, within the bound.
A program may use at most 192 MiB of HBM per device.

```python
import jax
import jax.numpy as jnp
from jax import lax

STATION_ANTENNAS = 256
SUBBAND_COUNT = 256
STATION_BEAMS = 32
TIME_SAMPLES = 128
STATION_COUNT = 16


def draw_antenna_flags(key, part):
    initial_key, second_key = jax.random.split(jax.random.fold_in(key, 11))
    antenna_indices = jnp.arange(STATION_ANTENNAS, dtype=jnp.int32)
    slope_level = 5 + 90 * antenna_indices // STATION_ANTENNAS
    cyclic_shifts = jax.random.randint(initial_key, (STATION_COUNT, STATION_ANTENNAS), 0, 100)
    comb_phase = jax.random.randint(second_key, (STATION_COUNT, 1), 0, 8)
    usable = (cyclic_shifts < slope_level[None, :]) | (antenna_indices[None, :] % 8 == comb_phase)
    return usable.astype(jnp.int32)


def levels(rng, extent, cuts, low, largest):
    loudness, own = 1.0, jax.random.fold_in(rng, 6)
    for position, blocks in cuts:
        heights = jnp.exp(jax.random.uniform(jax.random.fold_in(own, position), (blocks,), jnp.float32, low / len(cuts), largest / len(cuts)))
        loudness = loudness * jnp.repeat(heights, extent[position] // blocks).reshape([-1 if axis == position else 1 for axis in range(len(extent))])
    return loudness


def normal_values(key, dims, scale, bound, cuts=(), held_as=jnp.bfloat16):
    values = scale * jax.random.normal(key, dims, jnp.float32)
    if cuts:
        values = values * levels(key, dims, cuts, -0.22, 0.18)
    return jnp.clip(values, -bound, bound).astype(held_as)


def setup_inputs(seed: int = 0) -> dict:
    arg_keys = jax.random.split(jax.random.key(seed), 5)
    return {
        "samples": normal_values(arg_keys[0], (2, STATION_COUNT, STATION_ANTENNAS, TIME_SAMPLES, SUBBAND_COUNT), 1.0, 6.0, ((1, 16), (2, 2)), jnp.float32),
        "weights": normal_values(arg_keys[1], (2, STATION_COUNT, STATION_BEAMS, STATION_ANTENNAS, SUBBAND_COUNT), 1.0, 6.0, ((1, 16), (3, 2)), jnp.float32),
        "antenna_flags": draw_antenna_flags(jax.random.fold_in(arg_keys[4], 71), 0),
        "subband_table": jax.random.permutation(arg_keys[3], SUBBAND_COUNT).astype(jnp.int32),
    }


def contract_beam(steer, signal):
    return jnp.einsum('baf,atf->fbt', steer, signal, precision=lax.Precision.HIGHEST)

def contract_pair(left, right):
    return jnp.einsum('sfbt,rfbt->fsbr', left, right, precision=lax.Precision.HIGHEST)

def reference(samples, weights, antenna_flags, subband_table):
    usable = antenna_flags.astype(jnp.float32)
    gain_scale = lax.rsqrt(lax.optimization_barrier(jnp.sum(usable, axis=1)))

    def station_beams(packed):
        signal, steer, usable_row = packed
        signal = jnp.take(signal * usable_row[None, :, None, None], subband_table, axis=3)
        steer = jnp.take(steer, subband_table, axis=3)
        real_part = contract_beam(steer[0], signal[0]) - contract_beam(steer[1], signal[1])
        imag_part = contract_beam(steer[0], signal[1]) + contract_beam(steer[1], signal[0])
        return jnp.stack([real_part, imag_part], axis=1)
    beam_sum = lax.map(station_beams, (jnp.moveaxis(samples, 1, 0), jnp.moveaxis(weights, 1, 0), usable))
    beam_data = (beam_sum * gain_scale[:, None, None, None, None]).astype(jnp.bfloat16)
    signal = beam_data.astype(jnp.float32)
    real_part = contract_pair(signal[:, :, 0], signal[:, :, 0]) + contract_pair(signal[:, :, 1], signal[:, :, 1])
    imag_part = contract_pair(signal[:, :, 1], signal[:, :, 0]) - contract_pair(signal[:, :, 0], signal[:, :, 1])
    return jnp.stack([real_part, imag_part], axis=1)
```

```python
import jax
import jax.numpy as jnp
from jax import lax
from jax.sharding import PartitionSpec as P


def beamform(steer, signal):

    def contract(left, right):
        return jnp.einsum(
            "sabf,satf->fsbt",
            left,
            right,
            precision=lax.Precision.HIGHEST,
            preferred_element_type=jnp.float32,
        )

    real_part = contract(steer[0], signal[0]) - contract(steer[1], signal[1])
    imag_part = contract(steer[0], signal[1]) + contract(steer[1], signal[0])
    return jnp.stack([real_part, imag_part], axis=1)


def on_device(samples, weights, antenna_flags, subband_table):
    usable = antenna_flags.astype(jnp.float32)
    usable_count = lax.psum(jnp.sum(usable, axis=1), "chan")
    gain_scale = lax.rsqrt(usable_count)
    steer = jnp.swapaxes(weights, 2, 3) * usable[None, :, :, None, None]
    partial = jnp.take(beamform(steer, samples), subband_table, axis=0)[:, :, 0]
    groups = lax.axis_size("chan")
    mine = lax.axis_index("chan")
    partial = partial.reshape(groups, -1, *partial.shape[1:])
    arrived = lax.all_to_all(partial.astype(jnp.bfloat16), "chan", 0, 0)
    own = lax.dynamic_index_in_dim(partial, mine, 0, keepdims=False)
    is_mine = (jnp.arange(groups) == mine)[:, None, None, None, None]
    beam_sum = own + jnp.sum(jnp.where(is_mine, 0.0, arrived.astype(jnp.float32)), axis=0)
    beam_data = (beam_sum * gain_scale).astype(jnp.bfloat16)
    stations = lax.axis_size("station")
    spread = beam_data.reshape(stations, -1, *beam_data.shape[1:])
    gathered = lax.all_to_all(spread, "station", 0, 0)
    swapped = jnp.stack([gathered[:, :, 1], -gathered[:, :, 0]], axis=2)
    stacked = jnp.stack([gathered, swapped], axis=0)
    pairs = jnp.einsum("osfcbt,rfcbt->sfobr", stacked, gathered, preferred_element_type=jnp.float32)
    returned = lax.all_to_all(pairs, "station", 0, 0)
    return returned.reshape(-1, *returned.shape[2:])[:, :, None]


def solution(mesh):
    in_specs = (
        P(None, "station", "chan", None, None),
        P(None, "station", None, "chan", None),
        P("station", "chan"),
        P(),
    )
    out_specs = P("chan", None, "station", None, None)
    return jax.shard_map(
        on_device, mesh=mesh, in_specs=in_specs, out_specs=out_specs, check_vma=False
    )
```

```python
import functools

import jax
import jax.numpy as jnp
from jax import lax
from jax.experimental import pallas as pl
from jax.experimental.pallas import tpu as pltpu
from jax.sharding import PartitionSpec as P

LANES = 128
ANTENNAS_PER_STEP = 16
UNROLL = 4


def split(value):
    high = value.astype(jnp.bfloat16)
    low = (value - high.astype(jnp.float32)).astype(jnp.bfloat16)
    return high, low


def beam_kernel(table_ref, x_ref, w_ref, usable_ref, sent_ref, own_ref, slot_ref, x_rows, w_rows, *, antennas, beams):
    block, step = pl.program_id(0), pl.program_id(1)
    mine = lax.axis_index("chan")
    subbands = sent_ref.shape[0]
    kept = own_ref.shape[0] - 1
    x_stride = x_rows.shape[0] // LANES
    w_stride = w_rows.shape[0] // LANES
    x_step = x_ref.shape[2]
    w_step = w_ref.shape[2]

    @pl.when((block == 0) & (step == 0))
    def _():
        @pl.loop(0, subbands)
        def _(slot):
            slot_ref[table_ref[slot]] = slot

    for part in range(2):
        for a in range(x_step):
            row = part * antennas + step * x_step + a
            x_rows[pl.ds(row, LANES, stride=x_stride), :] = x_ref[part, 0, a].T
        for b in range(w_step):
            tile = w_ref[part, 0, b]
            if antennas < LANES:
                tile = jnp.concatenate([tile, jnp.zeros((LANES - antennas, LANES), jnp.float32)], axis=0)
            row = part * beams + step * w_step + b
            w_rows[pl.ds(row, LANES, stride=w_stride), :] = tile.T

    @pl.when(step == pl.num_programs(1) - 1)
    def _():
        usable = usable_ref[...]

        def one(f):
            x = x_rows[pl.ds(pl.multiple_of(f * x_stride, 8), 2 * antennas), :]
            w = w_rows[pl.ds(pl.multiple_of(f * w_stride, 8), 2 * beams), :][:, :antennas] * usable
            w_re, w_im = w[:beams], w[beams:]
            steer = jnp.concatenate(
                [jnp.concatenate([w_re, -w_im], axis=1), jnp.concatenate([w_im, w_re], axis=1)], axis=0
            )
            x_pair = jnp.concatenate(split(x), axis=1)
            w_pair = jnp.concatenate(split(steer), axis=0)
            grid = jnp.dot(w_pair, x_pair, preferred_element_type=jnp.float32)
            rows, cols = 2 * beams, x.shape[1]
            total = grid[:rows, :cols] + (grid[rows:, :cols] + grid[:rows, cols:] + grid[rows:, cols:])
            slot = slot_ref[block * LANES + f]
            sent_ref[slot] = total.astype(jnp.bfloat16)
            local = slot - mine * kept
            own_ref[jnp.where((local >= 0) & (local < kept), local, kept)] = total

        @pl.loop(0, LANES // UNROLL)
        def _(group):
            for u in range(UNROLL):
                one(group * UNROLL + u)


def beam_partials(samples, weights, usable, table, groups):
    _, _, antennas, times, subbands = samples.shape
    beams = weights.shape[2]
    steps = antennas // ANTENNAS_PER_STEP
    w_step = beams // steps
    grid_spec = pltpu.PrefetchScalarGridSpec(
        num_scalar_prefetch=1,
        grid=(subbands // LANES, steps),
        in_specs=[
            pl.BlockSpec((2, 1, ANTENNAS_PER_STEP, times, LANES), lambda f, s, *_: (0, 0, s, 0, f)),
            pl.BlockSpec((2, 1, w_step, antennas, LANES), lambda f, s, *_: (0, 0, s, 0, f)),
            pl.BlockSpec((1, antennas), lambda f, s, *_: (0, 0)),
        ],
        out_specs=[
            pl.BlockSpec((subbands, 2 * beams, times), lambda f, s, *_: (0, 0, 0)),
            pl.BlockSpec((subbands // groups + 1, 2 * beams, times), lambda f, s, *_: (0, 0, 0)),
        ],
        scratch_shapes=[
            pltpu.SMEM((subbands,), jnp.int32),
            pltpu.VMEM((LANES * (2 * antennas + 8), times), jnp.float32),
            pltpu.VMEM((LANES * (2 * beams + 8), LANES), jnp.float32),
        ],
    )
    return pl.pallas_call(
        functools.partial(beam_kernel, antennas=antennas, beams=beams),
        grid_spec=grid_spec,
        out_shape=[
            jax.ShapeDtypeStruct((subbands, 2 * beams, times), jnp.bfloat16),
            jax.ShapeDtypeStruct((subbands // groups + 1, 2 * beams, times), jnp.float32),
        ],
        compiler_params=pltpu.CompilerParams(
            dimension_semantics=("arbitrary", "arbitrary"), vmem_limit_bytes=60 * 1024 * 1024
        ),
    )(table, samples, weights, usable)


def on_device(samples, weights, antenna_flags, subband_table):
    usable = antenna_flags.astype(jnp.float32)
    usable_count = lax.psum(jnp.sum(usable, axis=1), "chan")
    gain_scale = lax.rsqrt(usable_count)
    groups = lax.axis_size("chan")
    mine = lax.axis_index("chan")
    beams, times = weights.shape[2], samples.shape[3]
    sent, own = beam_partials(samples, weights, usable, subband_table, groups)
    sent = sent.reshape(groups, -1, 2, beams, times)
    arrived = lax.all_to_all(sent, "chan", 0, 0)
    own = own[:-1].reshape(-1, 2, beams, times)
    is_mine = (jnp.arange(groups) == mine)[:, None, None, None, None]
    beam_sum = own + jnp.sum(jnp.where(is_mine, 0.0, arrived.astype(jnp.float32)), axis=0)
    beam_data = (beam_sum * gain_scale).astype(jnp.bfloat16)
    stations = lax.axis_size("station")
    spread = beam_data.reshape(stations, -1, *beam_data.shape[1:])
    gathered = lax.all_to_all(spread, "station", 0, 0)
    swapped = jnp.stack([gathered[:, :, 1], -gathered[:, :, 0]], axis=2)
    stacked = jnp.stack([gathered, swapped], axis=0)
    pairs = jnp.einsum("osfcbt,rfcbt->sfobr", stacked, gathered, preferred_element_type=jnp.float32)
    returned = lax.all_to_all(pairs, "station", 0, 0)
    return returned.reshape(-1, *returned.shape[2:])[:, :, None]


def solution(mesh):
    in_specs = (
        P(None, "station", "chan", None, None),
        P(None, "station", None, "chan", None),
        P("station", "chan"),
        P(),
    )
    out_specs = P("chan", None, "station", None, None)
    return jax.shard_map(
        on_device, mesh=mesh, in_specs=in_specs, out_specs=out_specs, check_vma=False
    )
```

```python
import functools

import jax
import jax.numpy as jnp
from jax import lax
from jax.experimental import pallas as pl
from jax.experimental.pallas import tpu as pltpu
from jax.sharding import PartitionSpec as P

LANES = 128
ANTENNAS_PER_STEP = 16
UNROLL = 4
STATIONS_PER_STEP = 4


def split(value):
    high = value.astype(jnp.bfloat16)
    low = (value - high.astype(jnp.float32)).astype(jnp.bfloat16)
    return high, low


def beam_kernel(table_ref, x_ref, w_ref, usable_ref, sent_ref, own_ref, slot_ref, x_rows, w_rows, *, antennas, beams):
    block, step = pl.program_id(0), pl.program_id(1)
    mine = lax.axis_index("chan")
    subbands = sent_ref.shape[0]
    kept = own_ref.shape[0] - 1
    x_stride = x_rows.shape[0] // LANES
    w_stride = w_rows.shape[0] // LANES
    x_step = x_ref.shape[2]
    w_step = w_ref.shape[2]

    @pl.when((block == 0) & (step == 0))
    def _():
        @pl.loop(0, subbands)
        def _(slot):
            slot_ref[table_ref[slot]] = slot

    for part in range(2):
        for a in range(x_step):
            row = part * antennas + step * x_step + a
            x_rows[pl.ds(row, LANES, stride=x_stride), :] = x_ref[part, 0, a].T
        for b in range(w_step):
            tile = w_ref[part, 0, b]
            if antennas < LANES:
                tile = jnp.concatenate([tile, jnp.zeros((LANES - antennas, LANES), jnp.float32)], axis=0)
            row = part * beams + step * w_step + b
            w_rows[pl.ds(row, LANES, stride=w_stride), :] = tile.T

    @pl.when(step == pl.num_programs(1) - 1)
    def _():
        usable = usable_ref[...]

        def one(f):
            x = x_rows[pl.ds(pl.multiple_of(f * x_stride, 8), 2 * antennas), :]
            w = w_rows[pl.ds(pl.multiple_of(f * w_stride, 8), 2 * beams), :][:, :antennas] * usable
            w_re, w_im = w[:beams], w[beams:]
            steer = jnp.concatenate(
                [jnp.concatenate([w_re, -w_im], axis=1), jnp.concatenate([w_im, w_re], axis=1)], axis=0
            )
            x_pair = jnp.concatenate(split(x), axis=1)
            w_pair = jnp.concatenate(split(steer), axis=0)
            grid = jnp.dot(w_pair, x_pair, preferred_element_type=jnp.float32)
            rows, cols = 2 * beams, x.shape[1]
            total = grid[:rows, :cols] + (grid[rows:, :cols] + grid[:rows, cols:] + grid[rows:, cols:])
            slot = slot_ref[block * LANES + f]
            sent_ref[slot] = total.astype(jnp.bfloat16)
            local = slot - mine * kept
            own_ref[jnp.where((local >= 0) & (local < kept), local, kept)] = total

        @pl.loop(0, LANES // UNROLL)
        def _(group):
            for u in range(UNROLL):
                one(group * UNROLL + u)


def beam_partials(samples, weights, usable, table, groups):
    _, _, antennas, times, subbands = samples.shape
    beams = weights.shape[2]
    steps = antennas // ANTENNAS_PER_STEP
    w_step = beams // steps
    grid_spec = pltpu.PrefetchScalarGridSpec(
        num_scalar_prefetch=1,
        grid=(subbands // LANES, steps),
        in_specs=[
            pl.BlockSpec((2, 1, ANTENNAS_PER_STEP, times, LANES), lambda f, s, *_: (0, 0, s, 0, f)),
            pl.BlockSpec((2, 1, w_step, antennas, LANES), lambda f, s, *_: (0, 0, s, 0, f)),
            pl.BlockSpec((1, antennas), lambda f, s, *_: (0, 0)),
        ],
        out_specs=[
            pl.BlockSpec((subbands, 2 * beams, times), lambda f, s, *_: (0, 0, 0)),
            pl.BlockSpec((subbands // groups + 1, 2 * beams, times), lambda f, s, *_: (0, 0, 0)),
        ],
        scratch_shapes=[
            pltpu.SMEM((subbands,), jnp.int32),
            pltpu.VMEM((LANES * (2 * antennas + 8), times), jnp.float32),
            pltpu.VMEM((LANES * (2 * beams + 8), LANES), jnp.float32),
        ],
    )
    return pl.pallas_call(
        functools.partial(beam_kernel, antennas=antennas, beams=beams),
        grid_spec=grid_spec,
        out_shape=[
            jax.ShapeDtypeStruct((subbands, 2 * beams, times), jnp.bfloat16),
            jax.ShapeDtypeStruct((subbands // groups + 1, 2 * beams, times), jnp.float32),
        ],
        compiler_params=pltpu.CompilerParams(
            dimension_semantics=("arbitrary", "arbitrary"), vmem_limit_bytes=60 * 1024 * 1024
        ),
    )(table, samples, weights, usable)


def exchange_kernel(
    sent_ref, own_hbm, count_ref, out_ref,
    own, arrived, outgoing, gathered, sums, returned, counts,
    own_sem, count_send, count_recv, chan_send, chan_recv, beam_send, beam_recv, back_send, back_recv,
):
    groups, stations = lax.axis_size("chan"), lax.axis_size("station")
    mine, me = lax.axis_index("chan"), lax.axis_index("station")
    phases, _, depth, rows, times = gathered.shape
    beams = rows // 2
    kept = own.shape[0]
    share = phases * depth
    wide = min(STATIONS_PER_STEP, stations)
    pieces = stations // wide

    def target(k):
        return lax.rem(me + stations // 2 + ((k + 1) // 2) * (1 - 2 * lax.rem(k, 2)), stations)

    def remote(src, dst, send, recv, device):
        return pltpu.make_async_remote_copy(
            src_ref=src, dst_ref=dst, send_sem=send, recv_sem=recv,
            device_id=device, device_id_type=pl.DeviceIdType.MESH,
        )

    def chan_copy(g, p, k):
        peer = lax.rem(mine + g, groups)
        start = peer * kept + target(k) * share + p * depth
        return remote(
            sent_ref.at[pl.ds(start, depth)], arrived.at[g - 1, p, k],
            chan_send.at[g - 1, p, k], chan_recv.at[g - 1, p, k], (me, peer),
        )

    def count_copy(g):
        return remote(
            count_ref, counts.at[g - 1], count_send.at[g - 1], count_recv.at[g - 1], (me, lax.rem(mine + g, groups))
        )

    def beam_copy(p, k):
        return remote(outgoing.at[p, k], gathered.at[p, me], beam_send.at[p, k], beam_recv.at[p, k], (target(k), mine))

    def back_copy(p, k):
        there = target(k)
        return remote(
            sums.at[p, pl.ds(pl.multiple_of(there * beams, beams), beams)],
            returned.at[p, me], back_send.at[p, k], back_recv.at[p, k], (there, mine),
        )

    load = pltpu.make_async_copy(own_hbm.at[pl.ds(0, kept)], own, own_sem)
    load.start()
    barrier = pltpu.get_barrier_semaphore()
    for g in range(1, groups):
        pl.semaphore_signal(
            barrier, inc=1, device_id=(me, lax.rem(mine + g, groups)), device_id_type=pl.DeviceIdType.MESH
        )

    @pl.loop(0, stations - 1)
    def _(k):
        pl.semaphore_signal(barrier, inc=1, device_id=(target(k), mine), device_id_type=pl.DeviceIdType.MESH)

    pl.semaphore_wait(barrier, groups - 1 + stations - 1)

    for g in range(1, groups):
        count_copy(g).start()
    for p in range(phases):
        @pl.loop(0, stations)
        def _(k):
            for g in range(1, groups):
                chan_copy(g, p, k).start()

    sums[...] = jnp.zeros_like(sums)
    load.wait()
    count = count_ref[...]
    for g in range(1, groups):
        count_copy(g).wait_recv()
        count = count + counts[g - 1]
    gain = lax.rsqrt(count)[0:1, :times].reshape(1, 1, times)

    def chunk(p, k):
        start = target(k) * share + p * depth
        total = own[pl.ds(start, depth)]
        for g in range(1, groups):
            chan_copy(g, p, k).wait_recv()
            total = total + arrived[g - 1, p, k].astype(jnp.float32)
        return (total * gain).astype(jnp.bfloat16)

    def forward(p, k):
        outgoing[p, k] = chunk(p, k)
        beam_copy(p, k).start()

    def forward_range(p, first, last, extra=None):
        @pl.loop(first, last)
        def _(k):
            forward(p, k)
            if extra is not None:
                extra(k)

    def keep(p):
        gathered[p, me] = chunk(p, stations - 1)

    def await_beams(p):
        @pl.loop(0, stations - 1)
        def _(k):
            beam_copy(p, k).wait_recv()

    columns = stations * beams
    lanes = sums.shape[2]

    def correlate(p, index):
        j, piece = index // pieces, lax.rem(index, pieces)

        def beams_of(stations_slice, count, part):
            return gathered[p, stations_slice, j, pl.ds(part * beams, beams), :].reshape(count * beams, times)

        some = pl.ds(piece * wide, wide)
        x_re, x_im = beams_of(some, wide, 0), beams_of(some, wide, 1)
        every = pl.ds(0, stations)
        y = jnp.concatenate([beams_of(every, stations, 0), beams_of(every, stations, 1)], axis=1)
        same = lax.rem(lax.broadcasted_iota(jnp.int32, (wide * beams, columns), 0), beams) == lax.rem(
            lax.broadcasted_iota(jnp.int32, (wide * beams, columns), 1), beams
        )
        station_of = lax.broadcasted_iota(jnp.int32, (columns, lanes), 0) // beams
        lane = lax.broadcasted_iota(jnp.int32, (columns, lanes), 1)
        where = pl.ds(pl.multiple_of(piece * (wide * beams), wide * beams), wide * beams)
        total = sums[p, where, :]
        for part, x in enumerate((jnp.concatenate([x_re, x_im], axis=1), jnp.concatenate([x_im, -x_re], axis=1))):
            pairs = lax.dot_general(x, y, (((1,), (1,)), ((), ())), preferred_element_type=jnp.float32)
            high, low = split(jnp.where(same, pairs, 0.0))
            place = (lane == station_of + (j * 2 + part) * stations).astype(jnp.float32).astype(jnp.bfloat16)
            total = total + (
                jnp.dot(high, place, preferred_element_type=jnp.float32)
                + jnp.dot(low, place, preferred_element_type=jnp.float32)
            )
        sums[p, where, :] = total

    def send_back(p):
        @pl.loop(0, stations - 1)
        def _(k):
            back_copy(p, k).start()

        returned[p, me] = sums[p, pl.ds(pl.multiple_of(me * beams, beams), beams), :]

    last = phases - 1
    for p in range(phases):
        if p == 0:
            forward_range(p, 0, stations - 1)
        else:
            quarter, half = stations // 4, stations // 2
            each = depth * pieces // half
            forward_range(p, 0, quarter)
            await_beams(p - 1)

            def extra(k):
                for c in range(each):
                    correlate(p - 1, (k - quarter) * each + c)

            forward_range(p, quarter, quarter + half, extra)
            send_back(p - 1)
            forward_range(p, quarter + half, stations - 1)
        keep(p)
    await_beams(last)

    @pl.loop(0, depth * pieces)
    def _(index):
        correlate(last, index)

    send_back(last)
    for p in range(phases):
        @pl.loop(0, stations - 1)
        def _(k):
            back_copy(p, k).wait_recv()
    out_ref[...] = returned[...]
    for g in range(1, groups):
        count_copy(g).wait_send()
    for p in range(phases):
        @pl.loop(0, stations)
        def _(k):
            for g in range(1, groups):
                chan_copy(g, p, k).wait_send()

        @pl.loop(0, stations - 1)
        def _(k):
            beam_copy(p, k).wait_send()
            back_copy(p, k).wait_send()


def exchange(sent, own, count, beams, groups, stations):
    subbands, rows, times = sent.shape
    kept = subbands // groups
    share = kept // stations
    phases = 2 if share % 4 == 0 else 1
    depth = share // phases
    lanes = depth * 2 * stations
    dma = pltpu.SemaphoreType.DMA
    return pl.pallas_call(
        exchange_kernel,
        out_shape=jax.ShapeDtypeStruct((phases, stations, beams, lanes), jnp.float32),
        in_specs=[
            pl.BlockSpec(memory_space=pl.ANY),
            pl.BlockSpec(memory_space=pl.ANY),
            pl.BlockSpec(memory_space=pltpu.VMEM),
        ],
        out_specs=pl.BlockSpec(memory_space=pltpu.VMEM),
        scratch_shapes=[
            pltpu.VMEM((kept, rows, times), jnp.float32),
            pltpu.VMEM((groups - 1, phases, stations, depth, rows, times), jnp.bfloat16),
            pltpu.VMEM((phases, stations, depth, rows, times), jnp.bfloat16),
            pltpu.VMEM((phases, stations, depth, rows, times), jnp.bfloat16),
            pltpu.VMEM((phases, stations * beams, lanes), jnp.float32),
            pltpu.VMEM((phases, stations, beams, lanes), jnp.float32),
            pltpu.VMEM((groups - 1, 8, LANES), jnp.float32),
            dma,
            dma((groups - 1,)),
            dma((groups - 1,)),
            dma((groups - 1, phases, stations)),
            dma((groups - 1, phases, stations)),
            dma((phases, stations)),
            dma((phases, stations)),
            dma((phases, stations)),
            dma((phases, stations)),
        ],
        compiler_params=pltpu.CompilerParams(
            collective_id=0, has_side_effects=True, vmem_limit_bytes=40 * 1024 * 1024
        ),
    )(sent, own, count)


def on_device(samples, weights, antenna_flags, subband_table):
    usable = antenna_flags.astype(jnp.float32)
    groups, stations = lax.axis_size("chan"), lax.axis_size("station")
    beams = weights.shape[2]
    sent, own = beam_partials(samples, weights, usable, subband_table, groups)
    count = jnp.broadcast_to(jnp.sum(usable, axis=1)[:, None], (8, LANES))
    back = exchange(sent, own, count, beams, groups, stations)
    phases = back.shape[0]
    back = back.reshape(phases, stations, beams, -1, 2, stations)
    back = back.transpose(1, 0, 3, 4, 2, 5)
    return back.reshape(-1, 2, 1, beams, stations)


def solution(mesh):
    in_specs = (
        P(None, "station", "chan", None, None),
        P(None, "station", None, "chan", None),
        P("station", "chan"),
        P(),
    )
    out_specs = P("chan", None, "station", None, None)
    return jax.shard_map(
        on_device, mesh=mesh, in_specs=in_specs, out_specs=out_specs, check_vma=False
    )
```

```python
import functools

import jax
import jax.numpy as jnp
from jax import lax
from jax.experimental import pallas as pl
from jax.experimental.pallas import tpu as pltpu
from jax.sharding import PartitionSpec as P

LANES = 128
ANTENNAS_PER_STEP = 32
UNROLL = 8
STATIONS_PER_STEP = 4


def split(value):
    high = value.astype(jnp.bfloat16)
    low = (value - high.astype(jnp.float32)).astype(jnp.bfloat16)
    return high, low


def beam_kernel(table_ref, x_ref, w_ref, usable_ref, sent_ref, own_ref, slot_ref, x_rows, w_rows, *, antennas, beams):
    block, step = pl.program_id(0), pl.program_id(1)
    mine = lax.axis_index("chan")
    subbands = sent_ref.shape[0]
    kept = own_ref.shape[0] - 1
    x_stride = x_rows.shape[0] // LANES
    w_stride = w_rows.shape[0] // LANES
    x_step = x_ref.shape[2]
    w_step = w_ref.shape[2]

    @pl.when((block == 0) & (step == 0))
    def _():
        @pl.loop(0, subbands)
        def _(slot):
            slot_ref[table_ref[slot]] = slot

    for part in range(2):
        for a in range(x_step):
            row = part * antennas + step * x_step + a
            x_rows[pl.ds(row, LANES, stride=x_stride), :] = x_ref[part, 0, a].T
        for b in range(w_step):
            tile = w_ref[part, 0, b]
            if antennas < LANES:
                tile = jnp.concatenate([tile, jnp.zeros((LANES - antennas, LANES), jnp.float32)], axis=0)
            row = part * beams + step * w_step + b
            w_rows[pl.ds(row, LANES, stride=w_stride), :] = tile.T

    @pl.when(step == pl.num_programs(1) - 1)
    def _():
        usable = usable_ref[...]

        def one(f):
            x = x_rows[pl.ds(pl.multiple_of(f * x_stride, 8), 2 * antennas), :]
            w = w_rows[pl.ds(pl.multiple_of(f * w_stride, 8), 2 * beams), :][:, :antennas] * usable
            w_re, w_im = w[:beams], w[beams:]
            steer = jnp.concatenate(
                [jnp.concatenate([w_re, -w_im], axis=1), jnp.concatenate([w_im, w_re], axis=1)], axis=0
            )
            x_pair = jnp.concatenate(split(x), axis=1)
            w_pair = jnp.concatenate(split(steer), axis=0)
            grid = jnp.dot(w_pair, x_pair, preferred_element_type=jnp.float32)
            rows, cols = 2 * beams, x.shape[1]
            total = grid[:rows, :cols] + (grid[rows:, :cols] + grid[:rows, cols:] + grid[rows:, cols:])
            slot = slot_ref[block * LANES + f]
            sent_ref[slot] = total.astype(jnp.bfloat16)
            local = slot - mine * kept
            own_ref[jnp.where((local >= 0) & (local < kept), local, kept)] = total

        @pl.loop(0, LANES // UNROLL)
        def _(group):
            for u in range(UNROLL):
                one(group * UNROLL + u)


def beam_partials(samples, weights, usable, table, groups):
    _, _, antennas, times, subbands = samples.shape
    beams = weights.shape[2]
    steps = antennas // ANTENNAS_PER_STEP
    w_step = beams // steps
    grid_spec = pltpu.PrefetchScalarGridSpec(
        num_scalar_prefetch=1,
        grid=(subbands // LANES, steps),
        in_specs=[
            pl.BlockSpec((2, 1, ANTENNAS_PER_STEP, times, LANES), lambda f, s, *_: (0, 0, s, 0, f)),
            pl.BlockSpec((2, 1, w_step, antennas, LANES), lambda f, s, *_: (0, 0, s, 0, f)),
            pl.BlockSpec((1, antennas), lambda f, s, *_: (0, 0)),
        ],
        out_specs=[
            pl.BlockSpec((subbands, 2 * beams, times), lambda f, s, *_: (0, 0, 0)),
            pl.BlockSpec((subbands // groups + 1, 2 * beams, times), lambda f, s, *_: (0, 0, 0)),
        ],
        scratch_shapes=[
            pltpu.SMEM((subbands,), jnp.int32),
            pltpu.VMEM((LANES * (2 * antennas + 8), times), jnp.float32),
            pltpu.VMEM((LANES * (2 * beams + 8), LANES), jnp.float32),
        ],
    )
    return pl.pallas_call(
        functools.partial(beam_kernel, antennas=antennas, beams=beams),
        grid_spec=grid_spec,
        out_shape=[
            jax.ShapeDtypeStruct((subbands, 2 * beams, times), jnp.bfloat16),
            jax.ShapeDtypeStruct((subbands // groups + 1, 2 * beams, times), jnp.float32),
        ],
        compiler_params=pltpu.CompilerParams(
            dimension_semantics=("arbitrary", "arbitrary"), vmem_limit_bytes=60 * 1024 * 1024
        ),
    )(table, samples, weights, usable)


def exchange_kernel(
    sent_ref, own_hbm, count_ref, out_ref,
    own, arrived, outgoing, gathered, sums, returned, counts,
    own_sem, count_send, count_recv, chan_send, chan_recv, beam_send, beam_recv, back_send, back_recv,
):
    groups, stations = lax.axis_size("chan"), lax.axis_size("station")
    mine, me = lax.axis_index("chan"), lax.axis_index("station")
    phases, _, depth, rows, times = gathered.shape
    beams = rows // 2
    kept = own.shape[0]
    share = phases * depth
    wide = min(STATIONS_PER_STEP, stations)
    pieces = stations // wide

    def target(k):
        return lax.rem(me + stations // 2 + ((k + 1) // 2) * (1 - 2 * lax.rem(k, 2)), stations)

    def remote(src, dst, send, recv, device):
        return pltpu.make_async_remote_copy(
            src_ref=src, dst_ref=dst, send_sem=send, recv_sem=recv,
            device_id=device, device_id_type=pl.DeviceIdType.MESH,
        )

    def chan_copy(g, p, k):
        peer = lax.rem(mine + g, groups)
        start = peer * kept + target(k) * share + p * depth
        return remote(
            sent_ref.at[pl.ds(start, depth)], arrived.at[g - 1, p, k],
            chan_send.at[g - 1, p, k], chan_recv.at[g - 1, p, k], (me, peer),
        )

    def count_copy(g):
        return remote(
            count_ref, counts.at[g - 1], count_send.at[g - 1], count_recv.at[g - 1], (me, lax.rem(mine + g, groups))
        )

    def beam_copy(p, k):
        return remote(outgoing.at[p, k], gathered.at[p, me], beam_send.at[p, k], beam_recv.at[p, k], (target(k), mine))

    def back_copy(p, k):
        there = target(k)
        return remote(
            sums.at[p, pl.ds(pl.multiple_of(there * beams, beams), beams)],
            returned.at[p, me], back_send.at[p, k], back_recv.at[p, k], (there, mine),
        )

    load = pltpu.make_async_copy(own_hbm.at[pl.ds(0, kept)], own, own_sem)
    load.start()
    barrier = pltpu.get_barrier_semaphore()
    for g in range(1, groups):
        pl.semaphore_signal(
            barrier, inc=1, device_id=(me, lax.rem(mine + g, groups)), device_id_type=pl.DeviceIdType.MESH
        )

    @pl.loop(0, stations - 1)
    def _(k):
        pl.semaphore_signal(barrier, inc=1, device_id=(target(k), mine), device_id_type=pl.DeviceIdType.MESH)

    pl.semaphore_wait(barrier, groups - 1 + stations - 1)

    for g in range(1, groups):
        count_copy(g).start()
    for p in range(phases):
        @pl.loop(0, stations)
        def _(k):
            for g in range(1, groups):
                chan_copy(g, p, k).start()

    sums[...] = jnp.zeros_like(sums)
    load.wait()
    count = count_ref[...]
    for g in range(1, groups):
        count_copy(g).wait_recv()
        count = count + counts[g - 1]
    gain = lax.rsqrt(count)[0:1, :times].reshape(1, 1, times)

    def chunk(p, k):
        start = target(k) * share + p * depth
        total = own[pl.ds(start, depth)]
        for g in range(1, groups):
            chan_copy(g, p, k).wait_recv()
            total = total + arrived[g - 1, p, k].astype(jnp.float32)
        return (total * gain).astype(jnp.bfloat16)

    def forward(p, k):
        outgoing[p, k] = chunk(p, k)
        beam_copy(p, k).start()

    def forward_range(p, first, last, extra=None):
        @pl.loop(first, last)
        def _(k):
            forward(p, k)
            if extra is not None:
                extra(k)

    def keep(p):
        gathered[p, me] = chunk(p, stations - 1)

    def await_beams(p):
        @pl.loop(0, stations - 1)
        def _(k):
            beam_copy(p, k).wait_recv()

    columns = stations * beams
    lanes = sums.shape[2]

    def correlate(p, index):
        j, piece = index // pieces, lax.rem(index, pieces)

        def beams_of(stations_slice, count, part):
            return gathered[p, stations_slice, j, pl.ds(part * beams, beams), :].reshape(count * beams, times)

        some = pl.ds(piece * wide, wide)
        x_re, x_im = beams_of(some, wide, 0), beams_of(some, wide, 1)
        every = pl.ds(0, stations)
        y = jnp.concatenate([beams_of(every, stations, 0), beams_of(every, stations, 1)], axis=1)
        same = lax.rem(lax.broadcasted_iota(jnp.int32, (wide * beams, columns), 0), beams) == lax.rem(
            lax.broadcasted_iota(jnp.int32, (wide * beams, columns), 1), beams
        )
        station_of = lax.broadcasted_iota(jnp.int32, (columns, lanes), 0) // beams
        lane = lax.broadcasted_iota(jnp.int32, (columns, lanes), 1)
        where = pl.ds(pl.multiple_of(piece * (wide * beams), wide * beams), wide * beams)
        total = sums[p, where, :]
        for part, x in enumerate((jnp.concatenate([x_re, x_im], axis=1), jnp.concatenate([x_im, -x_re], axis=1))):
            pairs = lax.dot_general(x, y, (((1,), (1,)), ((), ())), preferred_element_type=jnp.float32)
            high, low = split(jnp.where(same, pairs, 0.0))
            place = (lane == station_of + (j * 2 + part) * stations).astype(jnp.float32).astype(jnp.bfloat16)
            total = total + (
                jnp.dot(high, place, preferred_element_type=jnp.float32)
                + jnp.dot(low, place, preferred_element_type=jnp.float32)
            )
        sums[p, where, :] = total

    def send_back(p):
        @pl.loop(0, stations - 1)
        def _(k):
            back_copy(p, k).start()

        returned[p, me] = sums[p, pl.ds(pl.multiple_of(me * beams, beams), beams), :]

    last = phases - 1
    for p in range(phases):
        if p == 0:
            forward_range(p, 0, stations - 1)
        else:
            quarter, half = stations // 4, stations // 2
            each = depth * pieces // half
            forward_range(p, 0, quarter)
            await_beams(p - 1)

            def extra(k):
                for c in range(each):
                    correlate(p - 1, (k - quarter) * each + c)

            forward_range(p, quarter, quarter + half, extra)
            send_back(p - 1)
            forward_range(p, quarter + half, stations - 1)
        keep(p)
    await_beams(last)

    @pl.loop(0, depth * pieces)
    def _(index):
        correlate(last, index)

    send_back(last)
    for p in range(phases):
        @pl.loop(0, stations - 1)
        def _(k):
            back_copy(p, k).wait_recv()
    out_ref[...] = returned[...]
    for g in range(1, groups):
        count_copy(g).wait_send()
    for p in range(phases):
        @pl.loop(0, stations)
        def _(k):
            for g in range(1, groups):
                chan_copy(g, p, k).wait_send()

        @pl.loop(0, stations - 1)
        def _(k):
            beam_copy(p, k).wait_send()
            back_copy(p, k).wait_send()


def exchange(sent, own, count, beams, groups, stations):
    subbands, rows, times = sent.shape
    kept = subbands // groups
    share = kept // stations
    phases = 2 if share % 4 == 0 else 1
    depth = share // phases
    lanes = depth * 2 * stations
    dma = pltpu.SemaphoreType.DMA
    return pl.pallas_call(
        exchange_kernel,
        out_shape=jax.ShapeDtypeStruct((phases, stations, beams, lanes), jnp.float32),
        in_specs=[
            pl.BlockSpec(memory_space=pl.ANY),
            pl.BlockSpec(memory_space=pl.ANY),
            pl.BlockSpec(memory_space=pltpu.VMEM),
        ],
        out_specs=pl.BlockSpec(memory_space=pltpu.VMEM),
        scratch_shapes=[
            pltpu.VMEM((kept, rows, times), jnp.float32),
            pltpu.VMEM((groups - 1, phases, stations, depth, rows, times), jnp.bfloat16),
            pltpu.VMEM((phases, stations, depth, rows, times), jnp.bfloat16),
            pltpu.VMEM((phases, stations, depth, rows, times), jnp.bfloat16),
            pltpu.VMEM((phases, stations * beams, lanes), jnp.float32),
            pltpu.VMEM((phases, stations, beams, lanes), jnp.float32),
            pltpu.VMEM((groups - 1, 8, LANES), jnp.float32),
            dma,
            dma((groups - 1,)),
            dma((groups - 1,)),
            dma((groups - 1, phases, stations)),
            dma((groups - 1, phases, stations)),
            dma((phases, stations)),
            dma((phases, stations)),
            dma((phases, stations)),
            dma((phases, stations)),
        ],
        compiler_params=pltpu.CompilerParams(
            collective_id=0, has_side_effects=True, vmem_limit_bytes=62 * 1024 * 1024
        ),
    )(sent, own, count)


def on_device(samples, weights, antenna_flags, subband_table):
    usable = antenna_flags.astype(jnp.float32)
    groups, stations = lax.axis_size("chan"), lax.axis_size("station")
    beams = weights.shape[2]
    sent, own = beam_partials(samples, weights, usable, subband_table, groups)
    count = jnp.broadcast_to(jnp.sum(usable, axis=1)[:, None], (8, LANES))
    back = exchange(sent, own, count, beams, groups, stations)
    phases = back.shape[0]
    back = back.reshape(phases, stations, beams, -1, 2, stations)
    back = back.transpose(1, 0, 3, 4, 2, 5)
    return back.reshape(-1, 2, 1, beams, stations)


def solution(mesh):
    in_specs = (
        P(None, "station", "chan", None, None),
        P(None, "station", None, "chan", None),
        P("station", "chan"),
        P(),
    )
    out_specs = P("chan", None, "station", None, None)
    return jax.shard_map(
        on_device, mesh=mesh, in_specs=in_specs, out_specs=out_specs, check_vma=False
    )
```
